256 devices in a mesh: subj: 32 (over x, z_hi, y), vox: 8 (over z_lo, core).
Axes of the slice: x: 4, y: 4, z: 8 (z_hi: 2, z_lo: 4; z = z_hi * 4 + z_lo), core: 2. Of those that a mesh axis runs over, the one named last changes fastest.
Arguments:
- bold_series: float32 [32, 300, 65536], P('subj', None, 'vox')
- seed_index: int32 [256], replicated, may hold values from 0 to 65535
Outputs:
- group_z: float32 [65536, 256], P(('vox', 'subj'))
The draws below stay inside these ranges and needn't reach their ends.
All inputs are finite; a program needn't handle non-finite values.
Results may differ from the reference program's by a relative error of at most 0.00031.
Values may be sent and summed in bfloat16 or wider, within the bound.
A program may use at most 64 MiB of HBM per device.

```python
import math
import jax
import jax.numpy as jnp
from jax import lax

TIMEPOINTS = 300
SEEDS = 256
SUBJ = 32
VOXELS = 65536


def draw_bold_series(key, part):
    factors = 4
    subkeys = jax.random.split(key, 6)
    hidden_factors = jax.random.normal(subkeys[0], (SUBJ, factors, TIMEPOINTS), jnp.float32)
    common_component = jax.random.normal(subkeys[1], (factors, VOXELS), jnp.float32) * (0.8 / math.sqrt(factors))
    subject_specific = jax.random.normal(subkeys[2], (SUBJ, factors, VOXELS), jnp.float32) * (0.6 / math.sqrt(factors))
    signal_component = jnp.einsum('oju,ojf->ouf', hidden_factors, common_component[None] + subject_specific)
    noise_part = jax.random.normal(subkeys[3], (SUBJ, TIMEPOINTS, VOXELS), jnp.float32)
    scale_factors = jnp.exp(jax.random.uniform(subkeys[4], (SUBJ, 1, VOXELS), jnp.float32, 0.0, math.log(10.0)))
    offsets = jax.random.uniform(subkeys[5], (SUBJ, 1, VOXELS), jnp.float32, -5.0, 5.0)
    return offsets + scale_factors * (signal_component + noise_part)


def place_ends(drawn, rng, smallest, largest):
    longest = drawn.shape.index(max(drawn.shape))
    spots = []
    for shift in (0, 1):
        where = [jax.random.randint(jax.random.fold_in(rng, axis), (), 0, length) for axis, length in enumerate(drawn.shape)]
        where[longest] = (where[longest] + shift) % drawn.shape[longest]
        spots.append(tuple(where))
    return drawn.at[spots[0]].set(smallest).at[spots[1]].set(largest)


def setup_inputs(seed: int = 0) -> dict:
    arg_keys = jax.random.split(jax.random.key(seed), 3)
    return {
        "bold_series": draw_bold_series(jax.random.fold_in(arg_keys[2], 71), 0),
        "seed_index": place_ends(jax.random.randint(arg_keys[1], (SEEDS,), 0, VOXELS), jax.random.fold_in(arg_keys[1], 1), 0, VOXELS - 1).astype(jnp.int32),
    }


clip_limit = 0.99
epsilon = 1e-05

def normalize(series):
    demean_series = series - lax.optimization_barrier(jnp.mean(series, axis=0, keepdims=True))
    spread = lax.optimization_barrier(jnp.mean(demean_series * demean_series, axis=0, keepdims=True))
    return (demean_series * lax.rsqrt(spread + epsilon)).astype(jnp.bfloat16)

def arctanh_transform(cross_product, length):
    clipped = jnp.clip(cross_product * (1.0 / length), -clip_limit, clip_limit)
    return 0.5 * jnp.log((1.0 + clipped) / (1.0 - clipped))

def reference(bold_series, seed_index):
    length = bold_series.shape[1]

    def accumulate(summed, series):
        normed = normalize(series)
        seed_panel = jnp.take(normed, seed_index.astype(jnp.int32), axis=1)
        cross_product = lax.dot_general(normed, seed_panel, (((0,), (0,)), ((), ())), preferred_element_type=jnp.float32)
        return (summed + arctanh_transform(cross_product, length), None)
    start_sum = jnp.zeros((bold_series.shape[2], seed_index.shape[0]), jnp.float32)
    summed, unused = lax.scan(accumulate, start_sum, bold_series)
    return summed * (1.0 / SUBJ)
```

```python
import functools

import jax
import jax.numpy as jnp
from jax import lax
from jax.experimental import pallas as pl
from jax.experimental.pallas import tpu as pltpu
from jax.sharding import Mesh
from jax.sharding import PartitionSpec as P

AXES = ("x", "zh", "y", "zl", "c")
SUBJ = ("x", "zh", "y")
VOX = ("zl", "c")

CLIP = 0.99
EPS = 1e-05
LIMIT = 2.6466525

T = 300
TP = 320
PIECE = TP // 4
V = 8192
K = 256
TILE = 256
W = 1024
B = 512
H = K // 2
Q = K // 4
SLOTS = 8
SUBJECTS = 32

MESH = pl.DeviceIdType.MESH


def step_of(terms):
    return 32700.0 / (terms * LIMIT) ** 0.5


def encode(z, terms):
    root = z * lax.rsqrt(jnp.maximum(jnp.abs(z), 1e-30))
    return jnp.round(root * step_of(terms)).astype(jnp.int32).astype(jnp.int16)


def decode(q, terms):
    r = q.astype(jnp.int32).astype(jnp.float32)
    return r * jnp.abs(r) * (1.0 / step_of(terms) ** 2)


def fisher(cross):
    c = jnp.clip(cross * (1.0 / T), -CLIP, CLIP)
    return 0.5 * (jnp.log(1.0 + c) - jnp.log(1.0 - c))


def kernel(
    bold, seeds, out,
    raw, normed, acc, panel, pieces, mine, full, seed_t,
    zf, zq, z2, relay, got, s1, s1q, s1m, relay2, got2, s2, s2q, gotz,
    load_sem, rs_send, rs_recv, ag_send, ag_recv,
    a_send, a_recv, b_send, b_recv, z_send, z_recv,
):
    x, zh, y, zl, c = (lax.axis_index(a) for a in AXES)
    xp, xm = lax.rem(x + 1, 4), lax.rem(x + 3, 4)
    yp, ym = lax.rem(y + 1, 4), lax.rem(y + 3, 4)
    peers = [(dz, dc) for dz in range(4) for dc in range(2) if dz or dc]

    def group(dz, dc):
        return {"zl": lax.rem(zl + dz, 4), "c": lax.rem(c + dc, 2)}

    ahead = ({"x": xp}, {"y": yp})
    behind = ({"x": xm}, {"y": ym})
    across = {"zh": 1 - zh}

    barrier = pltpu.get_barrier_semaphore()
    everyone = [group(*p) for p in peers] + [*ahead, *behind, across]
    for other in everyone:
        pl.semaphore_signal(barrier, inc=1, device_id=other, device_id_type=MESH)

    def load(i):
        return pltpu.make_async_copy(
            bold.at[:, 0, pl.ds(pl.multiple_of(i * W, W), W)], raw.at[i], load_sem.at[i]
        )

    @pl.loop(0, V // W)
    def _(i):
        load(i).start()

    acc[...] = jnp.zeros_like(acc)
    anchor = (zl * 2 + c) * V

    @pl.loop(0, V // W)
    def _(i):
        load(i).wait()
        for j in range(W // B):
            series = raw[i, :, j * B : (j + 1) * B]
            center = series - jnp.sum(series, axis=0, keepdims=True) * (1.0 / T)
            spread = jnp.sum(center * center, axis=0, keepdims=True) * (1.0 / T)
            columns = pl.ds(pl.multiple_of(i * W + j * B, B), B)
            normed[pl.ds(T - T % 16, TP - T + T % 16), columns] = jnp.zeros(
                (TP - T + T % 16, B), jnp.bfloat16
            )
            normed[pl.ds(0, T), columns] = (center * lax.rsqrt(spread + EPS)).astype(
                jnp.bfloat16
            )
        ids = lax.broadcasted_iota(jnp.int32, (W, K), 0) + (anchor + i * W)
        chosen = jnp.where(ids == seeds[...], 1.0, 0.0).astype(jnp.bfloat16)
        acc[...] += jnp.dot(
            normed[:, pl.ds(pl.multiple_of(i * W, W), W)],
            chosen,
            preferred_element_type=jnp.float32,
        )

    for h in range(2):
        for p in range(4):
            panel[h, p] = acc[p * PIECE : (p + 1) * PIECE, h * H : (h + 1) * H].astype(
                jnp.bfloat16
            )

    pl.semaphore_wait(barrier, len(everyone))

    def scatter(n):
        to = group(*peers[n])
        return pltpu.make_async_remote_copy(
            src_ref=panel.at[to["c"], to["zl"]],
            dst_ref=pieces.at[n],
            send_sem=rs_send.at[n],
            recv_sem=rs_recv.at[n],
            device_id=to,
            device_id_type=MESH,
        )

    def share(n):
        return pltpu.make_async_remote_copy(
            src_ref=mine,
            dst_ref=full.at[c, zl],
            send_sem=ag_send.at[n],
            recv_sem=ag_recv.at[n],
            device_id=group(*peers[n]),
            device_id_type=MESH,
        )

    def shared(n):
        dz, dc = peers[n]
        return pltpu.make_async_remote_copy(
            src_ref=mine,
            dst_ref=full.at[lax.rem(c + 2 - dc, 2), lax.rem(zl + 4 - dz, 4)],
            send_sem=ag_send.at[n],
            recv_sem=ag_recv.at[n],
            device_id=group(dz, dc),
            device_id_type=MESH,
        )

    for n in range(len(peers)):
        scatter(n).start()
    total = panel[c, zl].astype(jnp.float32)
    for n in range(len(peers)):
        scatter(n).wait_recv()
        total += pieces[n].astype(jnp.float32)
    mine[...] = total.astype(jnp.bfloat16)
    full[c, zl] = mine[...]
    for n in range(len(peers)):
        share(n).start()
    for n in range(len(peers)):
        shared(n).wait_recv()
    for h in range(2):
        whole = jnp.concatenate(
            [full[h, p].astype(jnp.float32) for p in range(4)]
            + [jnp.zeros((384 - TP, H), jnp.float32)],
            axis=0,
        )
        seed_t[h] = whole.T.astype(jnp.bfloat16)
    for n in range(len(peers)):
        scatter(n).wait_send()
        share(n).wait_send()

    def turn(j):
        return lax.rem(2 - j + 3 * (j // 2) + 2 * (j // 3), 4)

    def z_of(h, i, role):
        far = (2, 1, 3, 0)[role]
        g, j = i // 4, lax.rem(i, 4)
        zt = lax.rem(zh + 1 + g, 2)
        if h == 0:
            xt, yt = lax.rem(x + far, 4), lax.rem(y + turn(j), 4)
        else:
            xt, yt = lax.rem(x + turn(j), 4), lax.rem(y + far, 4)
        s = (xt * 2 + zt) * 4 + yt
        columns = pl.ds(pl.multiple_of(s * TILE, TILE), TILE)
        cross = jnp.dot(
            seed_t[h][:, :TP], normed[:, columns], preferred_element_type=jnp.float32
        )
        return fisher(cross)

    def message(i, h, way, kind):
        n = (h * 2 + way) * 3 + kind
        source = z2.at[i, h, way] if kind == 2 else zq.at[i, h, way, kind]
        target = relay.at[i, h, way] if kind == 0 else got.at[i, h, way, kind - 1]
        return pltpu.make_async_remote_copy(
            src_ref=source,
            dst_ref=target,
            send_sem=a_send.at[i, n],
            recv_sem=a_recv.at[i, n],
            device_id=(ahead, behind)[way][h],
            device_id_type=MESH,
        )

    def compute(i):
        for h in range(2):
            z = z_of(h, i, 0)
            zq[i, h, 0, 0] = encode(z[:Q], 1)
            zq[i, h, 1, 0] = encode(z[Q:], 1)
            message(i, h, 0, 0).start()
            message(i, h, 1, 0).start()
        for h in range(2):
            z = z_of(h, i, 1)
            zf[i, h, 0] = z[:Q]
            zq[i, h, 0, 1] = encode(z[Q:], 1)
            message(i, h, 0, 1).start()
            z = z_of(h, i, 2)
            zq[i, h, 1, 1] = encode(z[:Q], 1)
            zf[i, h, 1] = z[Q:]
            message(i, h, 1, 1).start()
        for h in range(2):
            z = z_of(h, i, 3)
            s1[i, h] = z

    def forward(i):
        for h in range(2):
            for way in range(2):
                message(i, h, way, 0).wait_recv()
                z2[i, h, way] = encode(zf[i, h, way] + decode(relay[i, h, way], 1), 2)
                message(i, h, way, 2).start()

    def message2(g, h, way, kind):
        n = (h * 2 + way) * 3 + kind
        source = s1m.at[g, h, way] if kind == 2 else s1q.at[g, h, way, kind]
        target = relay2.at[g, h, way] if kind == 0 else got2.at[g, h, way, kind - 1]
        return pltpu.make_async_remote_copy(
            src_ref=source,
            dst_ref=target,
            send_sem=b_send.at[g, n],
            recv_sem=b_recv.at[g, n],
            device_id=(ahead, behind)[way][1 - h],
            device_id_type=MESH,
        )

    def gather_in(i):
        g, j = i // 4, lax.rem(i, 4)
        for h in range(2):
            for way in range(2):
                message(i, h, way, 1).wait_recv()
                message(i, h, way, 2).wait_recv()
            s1[i, h, :Q] += decode(got[i, h, 0, 1], 2) + decode(got[i, h, 1, 0], 1)
            s1[i, h, Q:] += decode(got[i, h, 0, 0], 1) + decode(got[i, h, 1, 1], 2)

        @pl.when(j == 0)
        def _():
            for h in range(2):
                s1q[g, h, 0, 0] = encode(s1[i, h, :Q], 4)
                s1q[g, h, 1, 0] = encode(s1[i, h, Q:], 4)
                message2(g, h, 0, 0).start()
                message2(g, h, 1, 0).start()

        @pl.when(j == 1)
        def _():
            for h in range(2):
                s1q[g, h, 0, 1] = encode(s1[i, h, Q:], 4)
                message2(g, h, 0, 1).start()

        @pl.when(j == 2)
        def _():
            for h in range(2):
                s1q[g, h, 1, 1] = encode(s1[i, h, :Q], 4)
                message2(g, h, 1, 1).start()
            for h in range(2):
                for way in range(2):
                    message2(g, h, way, 0).wait_recv()
                    rows = slice(0, Q) if way == 0 else slice(Q, H)
                    s1m[g, h, way] = encode(
                        s1[i - 1 + way, h, rows] + decode(relay2[g, h, way], 4), 8
                    )
                    message2(g, h, way, 2).start()

    def cross_z():
        return pltpu.make_async_remote_copy(
            src_ref=s2q,
            dst_ref=gotz,
            send_sem=z_send,
            recv_sem=z_recv,
            device_id=across,
            device_id_type=MESH,
        )

    def finish(g):
        i = g * 4 + 3
        for h in range(2):
            for way in range(2):
                message2(g, h, way, 1).wait_recv()
                message2(g, h, way, 2).wait_recv()
            s2[h, :Q] = (
                s1[i, h, :Q] + decode(got2[g, h, 0, 1], 8) + decode(got2[g, h, 1, 0], 4)
            )
            s2[h, Q:] = (
                s1[i, h, Q:] + decode(got2[g, h, 0, 0], 4) + decode(got2[g, h, 1, 1], 8)
            )

    @pl.loop(0, SLOTS + 3)
    def _(i):
        @pl.when(i < SLOTS)
        def _():
            compute(i)

        @pl.when((i >= 1) & (i < SLOTS + 1))
        def _():
            forward(i - 1)

        @pl.when((i >= 2) & (i < SLOTS + 2))
        def _():
            gather_in(i - 2)

        @pl.when(i == 6)
        def _():
            finish(0)
            for h in range(2):
                s2q[h] = encode(s2[h], 16)
            cross_z().start()

    finish(1)
    cross_z().wait_recv()
    for h in range(2):
        out[h] = s2[h] + decode(gotz[h], 16)

    @pl.loop(0, SLOTS)
    def _(i):
        for h in range(2):
            for way in range(2):
                for kind in range(3):
                    message(i, h, way, kind).wait_send()

    @pl.loop(0, 2)
    def _(g):
        for h in range(2):
            for way in range(2):
                for kind in range(3):
                    message2(g, h, way, kind).wait_send()

    cross_z().wait_send()


def body(bold_series, seed_index):
    bf16, f32, i16 = jnp.bfloat16, jnp.float32, jnp.int16
    dma = pltpu.SemaphoreType.DMA
    summed = pl.pallas_call(
        kernel,
        out_shape=jax.ShapeDtypeStruct((2, H, TILE), f32),
        in_specs=[
            pl.BlockSpec(memory_space=pl.ANY),
            pl.BlockSpec(memory_space=pltpu.VMEM),
        ],
        out_specs=pl.BlockSpec(memory_space=pltpu.VMEM),
        scratch_shapes=[
            pltpu.VMEM((V // W, T, W), f32),
            pltpu.VMEM((TP, V), bf16),
            pltpu.VMEM((TP, K), f32),
            pltpu.VMEM((2, 4, PIECE, H), bf16),
            pltpu.VMEM((7, PIECE, H), bf16),
            pltpu.VMEM((PIECE, H), bf16),
            pltpu.VMEM((2, 4, PIECE, H), bf16),
            pltpu.VMEM((2, H, 384), bf16),
            pltpu.VMEM((SLOTS, 2, 2, Q, TILE), f32),
            pltpu.VMEM((SLOTS, 2, 2, 2, Q, TILE), i16),
            pltpu.VMEM((SLOTS, 2, 2, Q, TILE), i16),
            pltpu.VMEM((SLOTS, 2, 2, Q, TILE), i16),
            pltpu.VMEM((SLOTS, 2, 2, 2, Q, TILE), i16),
            pltpu.VMEM((SLOTS, 2, H, TILE), f32),
            pltpu.VMEM((2, 2, 2, 2, Q, TILE), i16),
            pltpu.VMEM((2, 2, 2, Q, TILE), i16),
            pltpu.VMEM((2, 2, 2, Q, TILE), i16),
            pltpu.VMEM((2, 2, 2, 2, Q, TILE), i16),
            pltpu.VMEM((2, H, TILE), f32),
            pltpu.VMEM((2, H, TILE), i16),
            pltpu.VMEM((2, H, TILE), i16),
            dma((V // W,)),
            dma((7,)), dma((7,)), dma((7,)), dma((7,)),
            dma((SLOTS, 12)), dma((SLOTS, 12)),
            dma((2, 12)), dma((2, 12)),
            dma, dma,
        ],
        compiler_params=pltpu.CompilerParams(
            collective_id=0, has_side_effects=True, vmem_limit_bytes=60 * 2**20
        ),
        name="group_z",
    )(bold_series.reshape(T, 1, V), seed_index.reshape(1, K))
    return summed.reshape(K, TILE).T * (1.0 / SUBJECTS)


def solution(mesh):
    split = Mesh(mesh.devices.reshape(4, 2, 4, 4, 2), AXES)
    return jax.shard_map(
        body,
        mesh=split,
        in_specs=(P(SUBJ, None, VOX), P()),
        out_specs=P(VOX + SUBJ, None),
        check_vma=False,
    )
```

```python
import functools

import jax
import jax.numpy as jnp
from jax import lax
from jax.experimental import pallas as pl
from jax.experimental.pallas import tpu as pltpu
from jax.sharding import Mesh
from jax.sharding import PartitionSpec as P

AXES = ("x", "zh", "y", "zl", "c")
SUBJ = ("x", "zh", "y")
VOX = ("zl", "c")

CLIP = 0.99
EPS = 1e-05
LIMIT = 2.6466525

T = 300
TP = 304
PIECE = 80
V = 8192
K = 256
LENT = 2
TILE = 256
W = 1024
B = 512
H = K // 2
Q = K // 4
SUBJECTS = 32

MESH = pl.DeviceIdType.MESH


def step_of(terms):
    return 32700.0 / (terms * LIMIT) ** 0.5


def encode(z, terms):
    root = z * lax.rsqrt(jnp.maximum(jnp.abs(z), 1e-30))
    return jnp.round(root * step_of(terms)).astype(jnp.int32).astype(jnp.int16)


def code(c):
    return jnp.round(c * (32700.0 / CLIP)).astype(jnp.int32).astype(jnp.int16)


def plain(q):
    return q.astype(jnp.int32).astype(jnp.float32) * (CLIP / 32700.0)


def decode(q, terms):
    r = q.astype(jnp.int32).astype(jnp.float32)
    return r * jnp.abs(r) * (1.0 / step_of(terms) ** 2)


def clipped(cross):
    return jnp.clip(cross * (1.0 / T), -CLIP, CLIP)


def fisher(c):
    return 0.5 * (jnp.log(1.0 + c) - jnp.log(1.0 - c))


def kernel(
    bold, seeds, out,
    chosen_seeds, raw, normed, acc, panel, pieces, mine, full, theirs, seed_t, tiles,
    zf, m3, got, cq, gotd, s1, s1q, s1m, relay2, got2, s2, s2q, gotz,
    seed_sem, load_sem, rs_send, rs_recv, ag_send, ag_recv, p_send, p_recv, t_send, t_recv,
    a_send, a_recv, d_send, d_recv, b_send, b_recv, z_send, z_recv,
):
    x, zh, y, zl, c = (lax.axis_index(a) for a in AXES)
    side, place = zl // 2, lax.rem(zl, 2)

    def there(dz):
        return (3 - 3 * side, 2 - side, side * 2 + 1 - place, zl)[dz]

    peers = [(dz, dc) for dz in range(3) for dc in range(2)] + [(3, 1)]

    def group(dz, dc):
        return {"zl": there(dz), "c": lax.rem(c + dc, 2)}

    def step(g, way):
        return ({"x": lax.rem(x + 1 + 2 * way, 4)}, {"y": lax.rem(y + 1 + 2 * way, 4)})[g]

    across = {"zh": 1 - zh}

    barrier = pltpu.get_barrier_semaphore()
    everyone = [group(*p) for p in peers]
    everyone += [step(g, way) for g in range(2) for way in range(2)] + [across]
    for other in everyone:
        pl.semaphore_signal(barrier, inc=1, device_id=other, device_id_type=MESH)

    def turn(j):
        return lax.rem(2 - j + 3 * (j // 2) + 2 * (j // 3), 4)

    def plane(g):
        return lax.rem(zh + 1 + g, 2)

    def target(g, j, off):
        if g == 0:
            xt, yt = lax.rem(x + off, 4), lax.rem(y + turn(j), 4)
        else:
            xt, yt = lax.rem(x + turn(j), 4), lax.rem(y + off, 4)
        return (xt * 2 + plane(g)) * 4 + yt

    def line(p, g):
        return lax.rem(x + turn(p), 4) * 2 + plane(g)

    def load(p, g):
        first = pl.multiple_of(line(p, g) * W, W)
        return pltpu.make_async_copy(
            bold.at[:, 0, pl.ds(first, W)], raw.at[p, g], load_sem.at[p, g]
        )

    seed_copy = pltpu.make_async_copy(seeds, chosen_seeds, seed_sem)
    seed_copy.start()

    @pl.loop(0, 4)
    def _(p):
        for g in range(2):
            load(p, g).start()

    acc[...] = jnp.zeros_like(acc)

    def normalize(p, g):
        for j in range(W // B):
            series = raw[p, g, :, j * B : (j + 1) * B]
            center = series - jnp.sum(series, axis=0, keepdims=True) * (1.0 / T)
            spread = jnp.sum(center * center, axis=0, keepdims=True) * (1.0 / T)
            result = (center * lax.rsqrt(spread + EPS)).astype(jnp.bfloat16)
            for k in range(B // TILE):
                s = line(p, g) * 4 + j * (B // TILE) + k
                normed[s, T - T % 16 :] = jnp.zeros((TP - T + T % 16, TILE), jnp.bfloat16)
                normed[s, :T] = result[:, k * TILE : (k + 1) * TILE]

    def pick(p, g):
        ids = lax.broadcasted_iota(jnp.int32, (W, K), 0)
        wanted = chosen_seeds[...] - (zl * 2 + c) * V - line(p, g) * W
        chosen = jnp.where(ids == wanted, 1.0, 0.0).astype(jnp.bfloat16)
        total = acc[:TP]
        for k in range(W // TILE):
            total += jnp.dot(
                normed[line(p, g) * 4 + k],
                chosen[k * TILE : (k + 1) * TILE],
                preferred_element_type=jnp.float32,
            )
        acc[:TP] = total

    def leaf(i, kind, s, to):
        return pltpu.make_async_remote_copy(
            src_ref=normed.at[s],
            dst_ref=tiles.at[i, kind],
            send_sem=t_send.at[i, kind],
            recv_sem=t_recv.at[i, kind],
            device_id=to,
            device_id_type=MESH,
        )

    seed_copy.wait()

    @pl.loop(0, 4)
    def _(p):
        with jax.named_scope("loadwait"):
            load(p, 0).wait()
        normalize(p, 0)

        @pl.when(p == 0)
        def _():
            with jax.named_scope("barrier"):
                pl.semaphore_wait(barrier, len(everyone))
            for j in range(4):
                leaf(j, 0, target(0, j, 2), step(0, j % 2)).start()

        @pl.when(p == 1)
        def _():
            for j in range(1, LENT, 2):
                leaf(j, 1, target(0, j, 1), step(0, 0)).start()

        @pl.when(p == 2)
        def _():
            for j in range(0, LENT, 2):
                leaf(j, 1, target(0, j, 3), step(0, 1)).start()

        load(p, 1).wait()
        pick(p, 0)
        normalize(p, 1)
        way = lax.rem(p, 2)
        leaf(4 + p, 0, target(1, p, 2), step(1, way)).start()

        @pl.when(p < LENT)
        def _():
            leaf(4 + p, 1, target(1, p, 3 - 2 * way), step(1, 1 - way)).start()

        pick(p, 1)

    for h in range(2):
        for p in range(4):
            panel[h, p] = acc[p * PIECE : (p + 1) * PIECE, h * H : (h + 1) * H].astype(
                jnp.bfloat16
            )

    here = zl * 2 + c

    def scatter(n, source):
        to = group(*peers[n])
        return pltpu.make_async_remote_copy(
            src_ref=panel.at[to["c"], to["zl"]],
            dst_ref=pieces.at[source],
            send_sem=rs_send.at[n],
            recv_sem=rs_recv.at[source],
            device_id=to,
            device_id_type=MESH,
        )

    def share(n, source):
        return pltpu.make_async_remote_copy(
            src_ref=mine,
            dst_ref=full.at[lax.rem(source, 2), source // 2],
            send_sem=ag_send.at[n],
            recv_sem=ag_recv.at[source],
            device_id=group(*peers[n]),
            device_id_type=MESH,
        )

    for n in range(len(peers)):
        scatter(n, here).start()
    total = panel[c, zl].astype(jnp.float32)
    for n in range(len(peers)):
        source = lax.rem(here + 1 + n, 8)
        with jax.named_scope("rs_wait"):
            scatter(n, source).wait_recv()
        total += pieces[source].astype(jnp.float32)
    mine[...] = total.astype(jnp.bfloat16)
    full[c, zl] = mine[...]
    for n in range(len(peers)):
        share(n, here).start()

    def lend(g, way, source):
        spot = (lax.rem(source, 2), source // 2)
        return pltpu.make_async_remote_copy(
            src_ref=full.at[spot],
            dst_ref=theirs.at[g, way].at[spot],
            send_sem=p_send.at[g, way, source],
            recv_sem=p_recv.at[g, way, source],
            device_id=step(g, way),
            device_id_type=MESH,
        )

    def lend_all(source):
        for g in range(2):
            for way in range(2):
                lend(g, way, source).start()

    lend_all(here)
    for n, (dz, dc) in reversed(list(enumerate(peers))):
        source = there(dz) * 2 + lax.rem(c + dc, 2)
        with jax.named_scope("ag_wait"):
            share(n, source).wait_recv()
        lend_all(source)

    def turned(n, source):
        for h in range(2):
            whole = jnp.concatenate(
                [source[h, p].astype(jnp.float32) for p in range(4)]
                + [jnp.zeros((384 - 4 * PIECE, H), jnp.float32)],
                axis=0,
            )
            seed_t[n, h] = whole.T.astype(jnp.bfloat16)

    turned(0, full)

    def c_of(n, h, series):
        cross = jnp.dot(seed_t[n, h][:, :TP], series, preferred_element_type=jnp.float32)
        return clipped(cross)

    def z_of(n, h, series):
        return fisher(c_of(n, h, series))

    slots = [(g, w) for g in range(2) for w in range(2)]

    def direct(g, j, h):
        return pltpu.make_async_remote_copy(
            src_ref=cq.at[g * 4 + j, h],
            dst_ref=gotd.at[g * 4 + j, h],
            send_sem=d_send.at[g * 4 + j, h],
            recv_sem=d_recv.at[g * 4 + j, h],
            device_id=step(g, 1 - j % 2),
            device_id_type=MESH,
        )

    for g in range(2):
        for h in range(2):
            for j in range(LENT, 4):
                series = normed[target(g, j, 3 - 2 * (j % 2))]
                cq[g * 4 + j, h] = code(c_of(0, h, series))
            for j in range(LENT, 4):
                direct(g, j, h).start()

    with jax.named_scope("own"):

        @pl.loop(0, 2)
        def _(jj):
            for g, w in slots:
                j = 2 * jj + w
                for h in range(2):
                    zf[g * 4 + j, h] = z_of(0, h, normed[target(g, j, 1 + 2 * w)])
                    s1[g * 4 + j, h] = z_of(0, h, normed[target(g, j, 0)])

    def borrow(g):
        for way in range(2):
            with jax.named_scope("lendwait"):
                for source in range(8):
                    lend(g, way, source).wait_recv()
            turned(1 + 2 * g + way, theirs.at[g, way])

    def summed(g, j, h):
        return pltpu.make_async_remote_copy(
            src_ref=m3.at[g * 4 + j, h],
            dst_ref=got.at[g * 4 + j, h],
            send_sem=a_send.at[g * 4 + j, h],
            recv_sem=a_recv.at[g * 4 + j, h],
            device_id=step(g, j % 2),
            device_id_type=MESH,
        )

    def came(g, j, kind):
        return leaf(g * 4 + j, kind, 0, step(g, 0))

    def far(g, h):
        if h == 0:
            for j in range(4):
                came(g, j, 0).wait_recv()
        for j in range(4):
            i, w = g * 4 + j, j % 2
            m3[i, h] = encode(zf[i, h] + z_of(1 + 2 * g + w, h, tiles[i, 0]), 2)
        for j in range(4):
            summed(g, j, h).start()

    def near(g, h):
        for j in range(4):
            if h == 0 and j < LENT:
                came(g, j, 1).wait_recv()
            if j >= LENT:
                direct(g, j, h).wait_recv()
        for j in range(4):
            i, w = g * 4 + j, j % 2
            if j < LENT:
                s1[i, h] += z_of(2 + 2 * g - w, h, tiles[i, 1])
            else:
                s1[i, h] += fisher(plain(gotd[g * 4 + j, h]))

    rows = (slice(0, Q), slice(Q, H))

    def message2(g, h, way, kind):
        return pltpu.make_async_remote_copy(
            src_ref=s1m.at[g, h, way] if kind == 2 else s1q.at[g, h, way, kind],
            dst_ref=relay2.at[g, h, way] if kind == 0 else got2.at[g, h, way, kind - 1],
            send_sem=b_send.at[g, h, way, kind],
            recv_sem=b_recv.at[g, h, way, kind],
            device_id=step(1 - g, way),
            device_id_type=MESH,
        )

    def add_in(g, h, j):
        with jax.named_scope("m3wait"):
            summed(g, j, h).wait_recv()
        s1[g * 4 + j, h] += decode(got[g * 4 + j, h], 2)

    def cross_z(h):
        return pltpu.make_async_remote_copy(
            src_ref=s2q.at[h],
            dst_ref=gotz.at[h],
            send_sem=z_send.at[h],
            recv_sem=z_recv.at[h],
            device_id=across,
            device_id_type=MESH,
        )

    def second(g, h):
        add_in(g, h, 0)
        for way in range(2):
            s1q[g, h, way, 0] = encode(s1[g * 4, h, rows[way]], 4)
            message2(g, h, way, 0).start()
        add_in(g, h, 1)
        s1q[g, h, 0, 1] = encode(s1[g * 4 + 1, h, rows[1]], 4)
        message2(g, h, 0, 1).start()

    def third(g, h):
        add_in(g, h, 2)
        s1q[g, h, 1, 1] = encode(s1[g * 4 + 2, h, rows[0]], 4)
        message2(g, h, 1, 1).start()
        for way in range(2):
            with jax.named_scope("relaywait"):
                message2(g, h, way, 0).wait_recv()
            s1m[g, h, way] = encode(
                s1[g * 4 + 1 + way, h, rows[way]] + decode(relay2[g, h, way], 4), 8
            )
            message2(g, h, way, 2).start()
        add_in(g, h, 3)

    def finish(g, h):
        for way in range(2):
            with jax.named_scope("finwait"):
                message2(g, h, 1 - way, 1).wait_recv()
                message2(g, h, way, 2).wait_recv()
            s2[g, h, rows[way]] = (
                s1[g * 4 + 3, h, rows[way]]
                + decode(got2[g, h, 1 - way, 0], 4)
                + decode(got2[g, h, way, 1], 8)
            )
        if g == 0:
            s2q[h] = encode(s2[g, h], 16)
            cross_z(h).start()

    borrow(0)
    with jax.named_scope("far0"):
        far(0, 0)
        far(0, 1)
    borrow(1)
    far(1, 0)
    with jax.named_scope("near0"):
        near(0, 0)
        near(0, 1)
    second(0, 0)
    near(1, 0)
    second(0, 1)
    far(1, 1)
    third(0, 0)
    near(1, 1)
    second(1, 0)
    third(0, 1)
    finish(0, 0)
    second(1, 1)
    finish(0, 1)
    third(1, 0)
    third(1, 1)
    for h in range(2):
        finish(1, h)
        with jax.named_scope("zwait"):
            cross_z(h).wait_recv()
        out[:, h * H : (h + 1) * H] = (
            (s2[1, h] + decode(gotz[h], 16)) * (1.0 / SUBJECTS)
        ).T

    for n in range(len(peers)):
        scatter(n, here).wait_send()
        share(n, here).wait_send()
    for g in range(2):
        for way in range(2):
            for source in range(8):
                lend(g, way, source).wait_send()
            for h in range(2):
                for kind in range(3):
                    message2(g, h, way, kind).wait_send()
        for j in range(4):
            came(g, j, 0).wait_send()
            if j < LENT:
                came(g, j, 1).wait_send()
            for h in range(2):
                summed(g, j, h).wait_send()
                if j >= LENT:
                    direct(g, j, h).wait_send()
    for h in range(2):
        cross_z(h).wait_send()


def body(bold_series, seed_index):
    bf16, f32, i16 = jnp.bfloat16, jnp.float32, jnp.int16
    dma = pltpu.SemaphoreType.DMA
    return pl.pallas_call(
        kernel,
        out_shape=jax.ShapeDtypeStruct((TILE, K), f32),
        in_specs=[
            pl.BlockSpec(memory_space=pltpu.HBM),
            pl.BlockSpec(memory_space=pltpu.HBM),
        ],
        out_specs=pl.BlockSpec(memory_space=pltpu.VMEM),
        scratch_shapes=[
            pltpu.VMEM((1, K), jnp.int32),
            pltpu.VMEM((4, 2, T, W), f32),
            pltpu.VMEM((V // TILE, TP, TILE), bf16),
            pltpu.VMEM((4 * PIECE, K), f32),
            pltpu.VMEM((2, 4, PIECE, H), bf16),
            pltpu.VMEM((8, PIECE, H), bf16),
            pltpu.VMEM((PIECE, H), bf16),
            pltpu.VMEM((2, 4, PIECE, H), bf16),
            pltpu.VMEM((2, 2, 2, 4, PIECE, H), bf16),
            pltpu.VMEM((5, 2, H, 384), bf16),
            pltpu.VMEM((8, 2, TP, TILE), bf16),
            pltpu.VMEM((8, 2, H, TILE), f32),
            pltpu.VMEM((8, 2, H, TILE), i16),
            pltpu.VMEM((8, 2, H, TILE), i16),
            pltpu.VMEM((8, 2, H, TILE), i16),
            pltpu.VMEM((8, 2, H, TILE), i16),
            pltpu.VMEM((8, 2, H, TILE), f32),
            pltpu.VMEM((2, 2, 2, 2, Q, TILE), i16),
            pltpu.VMEM((2, 2, 2, Q, TILE), i16),
            pltpu.VMEM((2, 2, 2, Q, TILE), i16),
            pltpu.VMEM((2, 2, 2, 2, Q, TILE), i16),
            pltpu.VMEM((2, 2, H, TILE), f32),
            pltpu.VMEM((2, H, TILE), i16),
            pltpu.VMEM((2, H, TILE), i16),
            dma,
            dma((4, 2)),
            dma((7,)), dma((8,)), dma((7,)), dma((8,)),
            dma((2, 2, 8)), dma((2, 2, 8)), dma((8, 2)), dma((8, 2)),
            dma((8, 2)), dma((8, 2)), dma((8, 2)), dma((8, 2)),
            dma((2, 2, 2, 3)), dma((2, 2, 2, 3)),
            dma((2,)), dma((2,)),
        ],
        compiler_params=pltpu.CompilerParams(
            collective_id=0, has_side_effects=True, vmem_limit_bytes=50 * 2**20
        ),
        name="group_z",
    )(bold_series.reshape(T, 1, V), seed_index.reshape(1, K))


def solution(mesh):
    split = Mesh(mesh.devices.reshape(4, 2, 4, 4, 2), AXES)
    return jax.shard_map(
        body,
        mesh=split,
        in_specs=(P(SUBJ, None, VOX), P()),
        out_specs=P(VOX + SUBJ, None),
        check_vma=False,
    )
```

```python
import functools

import jax
import jax.numpy as jnp
from jax import lax
from jax.experimental import pallas as pl
from jax.experimental.pallas import tpu as pltpu
from jax.sharding import Mesh
from jax.sharding import PartitionSpec as P

AXES = ("x", "zh", "y", "zl", "c")
SUBJ = ("x", "zh", "y")
VOX = ("zl", "c")

CLIP = 0.99
EPS = 1e-05
LIMIT = 2.6466525

T = 300
TP = 304
PIECE = 80
V = 8192
K = 256
LENT = 3
TILE = 256
W = 1024
B = 512
H = K // 2
Q = K // 4
SUBJECTS = 32

MESH = pl.DeviceIdType.MESH


def step_of(terms):
    return 32700.0 / (terms * LIMIT) ** 0.5


def encode(z, terms):
    root = z * lax.rsqrt(jnp.maximum(jnp.abs(z), 1e-30))
    return jnp.round(root * step_of(terms)).astype(jnp.int32).astype(jnp.int16)


def code(c):
    return jnp.round(c * (32700.0 / CLIP)).astype(jnp.int32).astype(jnp.int16)


def plain(q):
    return q.astype(jnp.int32).astype(jnp.float32) * (CLIP / 32700.0)


def decode(q, terms):
    r = q.astype(jnp.int32).astype(jnp.float32)
    return r * jnp.abs(r) * (1.0 / step_of(terms) ** 2)


def clipped(cross):
    return jnp.clip(cross * (1.0 / T), -CLIP, CLIP)


def fisher(c):
    return 0.5 * (jnp.log(1.0 + c) - jnp.log(1.0 - c))


def kernel(
    bold, seeds, out,
    chosen_seeds, raw, normed, acc, panel, half, both, pieces, full, theirs, seed_t, tiles,
    zf, m3, got, cq, gotd, s1, s1q, s1m, relay2, got2, s2, s2q, gotz,
    seed_sem, load_sem, h_send, h_recv, rs_send, rs_recv, ag_send, ag_recv, c_send, p_send, p_recv, t_send, t_recv,
    a_send, a_recv, d_send, d_recv, b_send, b_recv, z_send, z_recv,
):
    x, zh, y, zl, c = (lax.axis_index(a) for a in AXES)
    side, place = zl // 2, lax.rem(zl, 2)

    def there(dz):
        return (3 - 3 * side, 2 - side, side * 2 + 1 - place, zl)[dz]

    def step(g, way):
        return ({"x": lax.rem(x + 1 + 2 * way, 4)}, {"y": lax.rem(y + 1 + 2 * way, 4)})[g]

    across = {"zh": 1 - zh}

    barrier = pltpu.get_barrier_semaphore()
    everyone = [{"zl": there(dz)} for dz in range(3)] + [{"c": 1 - c}]
    everyone += [step(g, way) for g in range(2) for way in range(2)] + [across]
    for other in everyone:
        pl.semaphore_signal(barrier, inc=1, device_id=other, device_id_type=MESH)

    def turn(j):
        if isinstance(j, int):
            return (2, 1, 3, 0)[j]
        return lax.rem(2 - j + 3 * (j // 2) + 2 * (j // 3), 4)

    def plane(g):
        return lax.rem(zh + 1 + g, 2)

    def target(g, j, off):
        if g == 0:
            xt, yt = lax.rem(x + off, 4), lax.rem(y + turn(j), 4)
        else:
            xt, yt = lax.rem(x + turn(j), 4), lax.rem(y + off, 4)
        return (xt * 2 + plane(g)) * 4 + yt

    def line(p, g):
        return lax.rem(x + turn(p), 4) * 2 + plane(g)

    def load(p, g):
        first = pl.multiple_of(line(p, g) * W, W)
        return pltpu.make_async_copy(
            bold.at[:, 0, pl.ds(first, W)], raw.at[p, g], load_sem.at[p, g]
        )

    seed_copy = pltpu.make_async_copy(seeds, chosen_seeds, seed_sem)
    seed_copy.start()

    @pl.loop(0, 4)
    def _(p):
        for g in range(2):
            load(p, g).start()

    acc[...] = jnp.zeros_like(acc)

    def normalize(p, g):
        for j in range(W // B):
            series = raw[p, g, :, j * B : (j + 1) * B]
            center = series - jnp.sum(series, axis=0, keepdims=True) * (1.0 / T)
            spread = jnp.sum(center * center, axis=0, keepdims=True) * (1.0 / T)
            result = (center * lax.rsqrt(spread + EPS)).astype(jnp.bfloat16)
            for k in range(B // TILE):
                s = line(p, g) * 4 + j * (B // TILE) + k
                normed[s, T - T % 16 :] = jnp.zeros((TP - T + T % 16, TILE), jnp.bfloat16)
                normed[s, :T] = result[:, k * TILE : (k + 1) * TILE]

    def pick(p, g):
        ids = lax.broadcasted_iota(jnp.int32, (W, K), 0)
        wanted = chosen_seeds[...] - (zl * 2 + c) * V - line(p, g) * W
        chosen = jnp.where(ids == wanted, 1.0, 0.0).astype(jnp.bfloat16)
        total = acc[:TP]
        for k in range(W // TILE):
            total += jnp.dot(
                normed[line(p, g) * 4 + k],
                chosen[k * TILE : (k + 1) * TILE],
                preferred_element_type=jnp.float32,
            )
        acc[:TP] = total

    def leaf(i, kind, s, to):
        return pltpu.make_async_remote_copy(
            src_ref=normed.at[s],
            dst_ref=tiles.at[i, kind],
            send_sem=t_send.at[i, kind],
            recv_sem=t_recv.at[i, kind],
            device_id=to,
            device_id_type=MESH,
        )

    seed_copy.wait()

    def give(p, g):
        if g == 1:
            leaf(4 + p, 0, target(1, p, 2), step(1, p % 2)).start()
            if p < LENT:
                leaf(4 + p, 1, target(1, p, 3 - 2 * (p % 2)), step(1, 1 - p % 2)).start()
        elif p == 0:
            for j in range(4):
                leaf(j, 0, target(0, j, 2), step(0, j % 2)).start()
        elif p < 3:
            for j in range(2 - p, LENT, 2):
                leaf(j, 1, target(0, j, 2 * p - 1), step(0, p - 1)).start()

    order = [(p, g) for p in range(4) for g in range(2)]
    for n, (p, g) in enumerate(order):
        with jax.named_scope("loadwait"):
            load(p, g).wait()
        if n:
            pick(*order[n - 1])
        normalize(p, g)
        if n == 0:
            with jax.named_scope("barrier"):
                pl.semaphore_wait(barrier, len(everyone))
        give(p, g)
    pick(*order[-1])

    for h in range(2):
        for p in range(4):
            panel[h, p] = acc[p * PIECE : (p + 1) * PIECE, h * H : (h + 1) * H].astype(
                jnp.bfloat16
            )

    here = zl * 2 + c

    partner = {"c": 1 - c}

    def halve():
        return pltpu.make_async_remote_copy(
            src_ref=panel.at[1 - c],
            dst_ref=half,
            send_sem=h_send,
            recv_sem=h_recv,
            device_id=partner,
            device_id_type=MESH,
        )

    def scatter(dz, source):
        return pltpu.make_async_remote_copy(
            src_ref=both.at[there(dz)],
            dst_ref=pieces.at[source],
            send_sem=rs_send.at[dz],
            recv_sem=rs_recv.at[source],
            device_id={"zl": there(dz)},
            device_id_type=MESH,
        )

    def share(dz, source):
        return pltpu.make_async_remote_copy(
            src_ref=full.at[c, zl],
            dst_ref=full.at[c, source],
            send_sem=ag_send.at[dz],
            recv_sem=ag_recv.at[source * 2 + c],
            device_id={"zl": there(dz)},
            device_id_type=MESH,
        )

    def copy_over(core, source):
        return pltpu.make_async_remote_copy(
            src_ref=full.at[core, source],
            dst_ref=full.at[core, source],
            send_sem=c_send.at[source],
            recv_sem=ag_recv.at[source * 2 + core],
            device_id=partner,
            device_id_type=MESH,
        )

    halve().start()
    halve().wait_recv()
    for p in range(4):
        both[p] = (panel[c, p].astype(jnp.float32) + half[p].astype(jnp.float32)).astype(
            jnp.bfloat16
        )
    for dz in range(3):
        scatter(dz, zl).start()
    total = both[zl].astype(jnp.float32)
    for dz in (2, 1, 0):
        with jax.named_scope("rs_wait"):
            scatter(dz, there(dz)).wait_recv()
        total += pieces[there(dz)].astype(jnp.float32)
    full[c, zl] = total.astype(jnp.bfloat16)
    for dz in range(3):
        share(dz, zl).start()
    copy_over(c, zl).start()

    def lend(g, way, source):
        spot = (lax.rem(source, 2), source // 2)
        return pltpu.make_async_remote_copy(
            src_ref=full.at[spot],
            dst_ref=theirs.at[g, way].at[spot],
            send_sem=p_send.at[g, way, source],
            recv_sem=p_recv.at[g, way, source],
            device_id=step(g, way),
            device_id_type=MESH,
        )

    def lend_all(source):
        for g in range(2):
            for way in range(2):
                lend(g, way, source).start()

    lend_all(here)
    for dz, core in ((3, 1), (2, 0), (2, 1), (1, 0), (0, 0), (1, 1), (0, 1)):
        source = there(dz)
        with jax.named_scope("ag_wait"):
            if core:
                copy_over(1 - c, source).wait_recv()
                lend_all(source * 2 + 1 - c)
            else:
                share(dz, source).wait_recv()
                copy_over(c, source).start()
                lend_all(source * 2 + c)

    def turned(n, source):
        for h in range(2):
            whole = jnp.concatenate(
                [source[h, p].astype(jnp.float32) for p in range(4)]
                + [jnp.zeros((384 - 4 * PIECE, H), jnp.float32)],
                axis=0,
            )
            seed_t[n, h] = whole.T.astype(jnp.bfloat16)

    turned(0, full)

    def c_of(n, h, series):
        cross = jnp.dot(seed_t[n, h][:, :TP], series, preferred_element_type=jnp.float32)
        return clipped(cross)

    def z_of(n, h, series):
        return fisher(c_of(n, h, series))

    slots = [(g, w) for g in range(2) for w in range(2)]

    def direct(g, j, h):
        return pltpu.make_async_remote_copy(
            src_ref=cq.at[g * 4 + j, h],
            dst_ref=gotd.at[g * 4 + j, h],
            send_sem=d_send.at[g * 4 + j, h],
            recv_sem=d_recv.at[g * 4 + j, h],
            device_id=step(g, 1 - j % 2),
            device_id_type=MESH,
        )

    for g in range(2):
        for h in range(2):
            for j in range(LENT, 4):
                series = normed[target(g, j, 3 - 2 * (j % 2))]
                cq[g * 4 + j, h] = code(c_of(0, h, series))
        for h in range(2):
            for j in range(LENT, 4):
                direct(g, j, h).start()

    with jax.named_scope("own"):

        @pl.loop(0, 2)
        def _(jj):
            for g, w in slots:
                j = 2 * jj + w
                for h in range(2):
                    zf[g * 4 + j, h] = z_of(0, h, normed[target(g, j, 1 + 2 * w)])

    def borrow(g):
        for way in range(2):
            with jax.named_scope("lendwait"):
                for source in range(8):
                    lend(g, way, source).wait_recv()
            turned(1 + 2 * g + way, theirs.at[g, way])

    def summed(g, j, h):
        return pltpu.make_async_remote_copy(
            src_ref=m3.at[g * 4 + j, h],
            dst_ref=got.at[g * 4 + j, h],
            send_sem=a_send.at[g * 4 + j, h],
            recv_sem=a_recv.at[g * 4 + j, h],
            device_id=step(g, j % 2),
            device_id_type=MESH,
        )

    def came(g, j, kind):
        return leaf(g * 4 + j, kind, 0, step(g, 0))

    def far(g, h):
        if h == 0:
            for j in range(4):
                came(g, j, 0).wait_recv()
        for j in range(4):
            i, w = g * 4 + j, j % 2
            m3[i, h] = encode(zf[i, h] + z_of(1 + 2 * g + w, h, tiles[i, 0]), 2)
        for j in range(4):
            summed(g, j, h).start()

    def near(g, h):
        for j in range(4):
            if h == 0 and j < LENT:
                came(g, j, 1).wait_recv()
            if j >= LENT:
                direct(g, j, h).wait_recv()
        for j in range(4):
            i, w = g * 4 + j, j % 2
            if j < LENT:
                term = z_of(2 + 2 * g - w, h, tiles[i, 1])
            else:
                term = fisher(plain(gotd[i, h]))
            s1[i, h] = z_of(0, h, normed[target(g, j, 0)]) + term

    rows = (slice(0, Q), slice(Q, H))

    def message2(g, h, way, kind):
        return pltpu.make_async_remote_copy(
            src_ref=s1m.at[g, h, way] if kind == 2 else s1q.at[g, h, way, kind],
            dst_ref=relay2.at[g, h, way] if kind == 0 else got2.at[g, h, way, kind - 1],
            send_sem=b_send.at[g, h, way, kind],
            recv_sem=b_recv.at[g, h, way, kind],
            device_id=step(1 - g, way),
            device_id_type=MESH,
        )

    def add_in(g, h, j):
        with jax.named_scope("m3wait"):
            summed(g, j, h).wait_recv()
        s1[g * 4 + j, h] += decode(got[g * 4 + j, h], 2)

    def cross_z(h):
        return pltpu.make_async_remote_copy(
            src_ref=s2q.at[h],
            dst_ref=gotz.at[h],
            send_sem=z_send.at[h],
            recv_sem=z_recv.at[h],
            device_id=across,
            device_id_type=MESH,
        )

    def second(g, h):
        add_in(g, h, 0)
        for way in range(2):
            s1q[g, h, way, 0] = encode(s1[g * 4, h, rows[way]], 4)
            message2(g, h, way, 0).start()
        add_in(g, h, 1)
        s1q[g, h, 0, 1] = encode(s1[g * 4 + 1, h, rows[1]], 4)
        message2(g, h, 0, 1).start()

    def third(g, h):
        add_in(g, h, 2)
        s1q[g, h, 1, 1] = encode(s1[g * 4 + 2, h, rows[0]], 4)
        message2(g, h, 1, 1).start()
        for way in range(2):
            with jax.named_scope("relaywait"):
                message2(g, h, way, 0).wait_recv()
            s1m[g, h, way] = encode(
                s1[g * 4 + 1 + way, h, rows[way]] + decode(relay2[g, h, way], 4), 8
            )
            message2(g, h, way, 2).start()
        add_in(g, h, 3)

    def finish(g, h):
        for way in range(2):
            with jax.named_scope("finwait"):
                message2(g, h, 1 - way, 1).wait_recv()
                message2(g, h, way, 2).wait_recv()
            s2[g, h, rows[way]] = (
                s1[g * 4 + 3, h, rows[way]]
                + decode(got2[g, h, 1 - way, 0], 4)
                + decode(got2[g, h, way, 1], 8)
            )
        if g == 0:
            s2q[h] = encode(s2[g, h], 16)
            cross_z(h).start()

    borrow(0)
    with jax.named_scope("far0"):
        far(0, 0)
        far(0, 1)
    borrow(1)
    far(1, 0)
    with jax.named_scope("near0"):
        near(0, 0)
        near(0, 1)
    second(0, 0)
    near(1, 0)
    second(0, 1)
    third(0, 0)
    far(1, 1)
    near(1, 1)
    second(1, 0)
    third(0, 1)
    finish(0, 0)
    second(1, 1)
    finish(0, 1)
    third(1, 0)
    third(1, 1)
    for h in range(2):
        finish(1, h)
        with jax.named_scope("zwait"):
            cross_z(h).wait_recv()
        out[:, h * H : (h + 1) * H] = (
            (s2[1, h] + decode(gotz[h], 16)) * (1.0 / SUBJECTS)
        ).T

    halve().wait_send()
    for dz in range(3):
        scatter(dz, zl).wait_send()
        share(dz, zl).wait_send()
    for source in range(4):
        copy_over(c, source).wait_send()
    for g in range(2):
        for way in range(2):
            for source in range(8):
                lend(g, way, source).wait_send()
            for h in range(2):
                for kind in range(3):
                    message2(g, h, way, kind).wait_send()
        for j in range(4):
            came(g, j, 0).wait_send()
            if j < LENT:
                came(g, j, 1).wait_send()
            for h in range(2):
                summed(g, j, h).wait_send()
                if j >= LENT:
                    direct(g, j, h).wait_send()
    for h in range(2):
        cross_z(h).wait_send()


def body(bold_series, seed_index):
    bf16, f32, i16 = jnp.bfloat16, jnp.float32, jnp.int16
    dma = pltpu.SemaphoreType.DMA
    return pl.pallas_call(
        kernel,
        out_shape=jax.ShapeDtypeStruct((TILE, K), f32),
        in_specs=[
            pl.BlockSpec(memory_space=pltpu.HBM),
            pl.BlockSpec(memory_space=pltpu.HBM),
        ],
        out_specs=pl.BlockSpec(memory_space=pltpu.VMEM),
        scratch_shapes=[
            pltpu.VMEM((1, K), jnp.int32),
            pltpu.VMEM((4, 2, T, W), f32),
            pltpu.VMEM((V // TILE, TP, TILE), bf16),
            pltpu.VMEM((4 * PIECE, K), f32),
            pltpu.VMEM((2, 4, PIECE, H), bf16),
            pltpu.VMEM((4, PIECE, H), bf16),
            pltpu.VMEM((4, PIECE, H), bf16),
            pltpu.VMEM((4, PIECE, H), bf16),
            pltpu.VMEM((2, 4, PIECE, H), bf16),
            pltpu.VMEM((2, 2, 2, 4, PIECE, H), bf16),
            pltpu.VMEM((5, 2, H, 384), bf16),
            pltpu.VMEM((8, 2, TP, TILE), bf16),
            pltpu.VMEM((8, 2, H, TILE), f32),
            pltpu.VMEM((8, 2, H, TILE), i16),
            pltpu.VMEM((8, 2, H, TILE), i16),
            pltpu.VMEM((8, 2, H, TILE), i16),
            pltpu.VMEM((8, 2, H, TILE), i16),
            pltpu.VMEM((8, 2, H, TILE), f32),
            pltpu.VMEM((2, 2, 2, 2, Q, TILE), i16),
            pltpu.VMEM((2, 2, 2, Q, TILE), i16),
            pltpu.VMEM((2, 2, 2, Q, TILE), i16),
            pltpu.VMEM((2, 2, 2, 2, Q, TILE), i16),
            pltpu.VMEM((2, 2, H, TILE), f32),
            pltpu.VMEM((2, H, TILE), i16),
            pltpu.VMEM((2, H, TILE), i16),
            dma,
            dma((4, 2)),
            dma, dma,
            dma((3,)), dma((4,)), dma((3,)), dma((8,)), dma((4,)),
            dma((2, 2, 8)), dma((2, 2, 8)), dma((8, 2)), dma((8, 2)),
            dma((8, 2)), dma((8, 2)), dma((8, 2)), dma((8, 2)),
            dma((2, 2, 2, 3)), dma((2, 2, 2, 3)),
            dma((2,)), dma((2,)),
        ],
        compiler_params=pltpu.CompilerParams(
            collective_id=0, has_side_effects=True, vmem_limit_bytes=50 * 2**20
        ),
        name="group_z",
    )(bold_series.reshape(T, 1, V), seed_index.reshape(1, K))


def solution(mesh):
    split = Mesh(mesh.devices.reshape(4, 2, 4, 4, 2), AXES)
    return jax.shard_map(
        body,
        mesh=split,
        in_specs=(P(SUBJ, None, VOX), P()),
        out_specs=P(VOX + SUBJ, None),
        check_vma=False,
    )
```

```python
import functools

import jax
import jax.numpy as jnp
from jax import lax
from jax.experimental import pallas as pl
from jax.experimental.pallas import tpu as pltpu
from jax.sharding import Mesh
from jax.sharding import PartitionSpec as P

AXES = ("x", "zh", "y", "zl", "c")
SUBJ = ("x", "zh", "y")
VOX = ("zl", "c")

CLIP = 0.99
EPS = 1e-05
LIMIT = 2.6466525

T = 300
TP = 304
PIECE = 80
V = 8192
K = 256
LENT = 3
TILE = 256
W = 1024
B = 512
H = K // 2
Q = K // 4
SUBJECTS = 32

MESH = pl.DeviceIdType.MESH


def step_of(terms):
    return 32700.0 / (terms * LIMIT) ** 0.5


def encode(z, terms):
    root = z * lax.rsqrt(jnp.maximum(jnp.abs(z), 1e-30))
    return jnp.round(root * step_of(terms)).astype(jnp.int32).astype(jnp.int16)


def code(c):
    return jnp.round(c * (32700.0 / CLIP)).astype(jnp.int32).astype(jnp.int16)


def plain(q):
    return q.astype(jnp.int32).astype(jnp.float32) * (CLIP / 32700.0)


def decode(q, terms):
    r = q.astype(jnp.int32).astype(jnp.float32)
    return r * jnp.abs(r) * (1.0 / step_of(terms) ** 2)


def clipped(cross):
    return jnp.clip(cross * (1.0 / T), -CLIP, CLIP)


def fisher(c):
    return 0.5 * (jnp.log(1.0 + c) - jnp.log(1.0 - c))


def kernel(
    bold, seeds, out,
    chosen_seeds, raw, normed, acc, panel, half, both, pieces, full, theirs, seed_t, tiles,
    zf, m3, got, cq, gotd, s1, s1q, s1m, relay2, got2, s2, s2q, gotz,
    seed_sem, load_sem, h_send, h_recv, rs_send, rs_recv, ag_send, ag_recv, c_send, p_send, p_recv, t_send, t_recv,
    a_send, a_recv, d_send, d_recv, b_send, b_recv, z_send, z_recv,
):
    x, zh, y, zl, c = (lax.axis_index(a) for a in AXES)
    side, place = zl // 2, lax.rem(zl, 2)

    def there(dz):
        return (3 - 3 * side, 2 - side, side * 2 + 1 - place, zl)[dz]

    def step(g, way):
        return ({"x": lax.rem(x + 1 + 2 * way, 4)}, {"y": lax.rem(y + 1 + 2 * way, 4)})[g]

    across = {"zh": 1 - zh}

    barrier = pltpu.get_barrier_semaphore()
    everyone = [{"zl": there(dz)} for dz in range(3)] + [{"c": 1 - c}]
    everyone += [step(g, way) for g in range(2) for way in range(2)] + [across]
    for other in everyone:
        pl.semaphore_signal(barrier, inc=1, device_id=other, device_id_type=MESH)

    def turn(j):
        if isinstance(j, int):
            return (2, 1, 3, 0)[j]
        return lax.rem(2 - j + 3 * (j // 2) + 2 * (j // 3), 4)

    def plane(g):
        return lax.rem(zh + 1 + g, 2)

    def target(g, j, off):
        if g == 0:
            xt, yt = lax.rem(x + off, 4), lax.rem(y + turn(j), 4)
        else:
            xt, yt = lax.rem(x + turn(j), 4), lax.rem(y + off, 4)
        return (xt * 2 + plane(g)) * 4 + yt

    def line(p, g):
        return lax.rem(x + turn(p), 4) * 2 + plane(g)

    def load(p, g):
        first = pl.multiple_of(line(p, g) * W, W)
        return pltpu.make_async_copy(
            bold.at[:, 0, pl.ds(first, W)], raw.at[p, g], load_sem.at[p, g]
        )

    seed_copy = pltpu.make_async_copy(seeds, chosen_seeds, seed_sem)
    seed_copy.start()

    @pl.loop(0, 4)
    def _(p):
        for g in range(2):
            load(p, g).start()

    acc[...] = jnp.zeros_like(acc)

    def normalize(p, g):
        for j in range(W // B):
            series = raw[p, g, :, j * B : (j + 1) * B]
            center = series - jnp.sum(series, axis=0, keepdims=True) * (1.0 / T)
            spread = jnp.sum(center * center, axis=0, keepdims=True) * (1.0 / T)
            result = (center * lax.rsqrt(spread + EPS)).astype(jnp.bfloat16)
            for k in range(B // TILE):
                s = line(p, g) * 4 + j * (B // TILE) + k
                normed[s, T - T % 16 :] = jnp.zeros((TP - T + T % 16, TILE), jnp.bfloat16)
                normed[s, :T] = result[:, k * TILE : (k + 1) * TILE]

    def pick(p, g):
        ids = lax.broadcasted_iota(jnp.int32, (W, K), 0)
        wanted = chosen_seeds[...] - (zl * 2 + c) * V - line(p, g) * W
        chosen = jnp.where(ids == wanted, 1.0, 0.0).astype(jnp.bfloat16)
        total = acc[:TP]
        for k in range(W // TILE):
            total += jnp.dot(
                normed[line(p, g) * 4 + k],
                chosen[k * TILE : (k + 1) * TILE],
                preferred_element_type=jnp.float32,
            )
        acc[:TP] = total

    def leaf(i, kind, s, to):
        return pltpu.make_async_remote_copy(
            src_ref=normed.at[s],
            dst_ref=tiles.at[i, kind],
            send_sem=t_send.at[i, kind],
            recv_sem=t_recv.at[i, kind],
            device_id=to,
            device_id_type=MESH,
        )

    seed_copy.wait()

    def give(p, g):
        if g == 1:
            leaf(4 + p, 0, target(1, p, 2), step(1, p % 2)).start()
            if p < LENT:
                leaf(4 + p, 1, target(1, p, 3 - 2 * (p % 2)), step(1, 1 - p % 2)).start()
        elif p == 0:
            for j in range(4):
                leaf(j, 0, target(0, j, 2), step(0, j % 2)).start()
        elif p < 3:
            for j in range(2 - p, LENT, 2):
                leaf(j, 1, target(0, j, 2 * p - 1), step(0, p - 1)).start()

    order = [(p, g) for p in range(4) for g in range(2)]
    for n, (p, g) in enumerate(order):
        with jax.named_scope("loadwait"):
            load(p, g).wait()
        if n:
            pick(*order[n - 1])
        normalize(p, g)
        if n == 0:
            with jax.named_scope("barrier"):
                pl.semaphore_wait(barrier, len(everyone))
        give(p, g)
    pick(*order[-1])

    for h in range(2):
        for p in range(4):
            panel[h, p] = acc[p * PIECE : (p + 1) * PIECE, h * H : (h + 1) * H].astype(
                jnp.bfloat16
            )

    here = zl * 2 + c

    partner = {"c": 1 - c}

    def halve():
        return pltpu.make_async_remote_copy(
            src_ref=panel.at[1 - c],
            dst_ref=half,
            send_sem=h_send,
            recv_sem=h_recv,
            device_id=partner,
            device_id_type=MESH,
        )

    def scatter(dz, source):
        return pltpu.make_async_remote_copy(
            src_ref=both.at[there(dz)],
            dst_ref=pieces.at[source],
            send_sem=rs_send.at[dz],
            recv_sem=rs_recv.at[source],
            device_id={"zl": there(dz)},
            device_id_type=MESH,
        )

    def share(dz, source):
        return pltpu.make_async_remote_copy(
            src_ref=full.at[c, zl],
            dst_ref=full.at[c, source],
            send_sem=ag_send.at[dz],
            recv_sem=ag_recv.at[source * 2 + c],
            device_id={"zl": there(dz)},
            device_id_type=MESH,
        )

    def copy_over(core, source):
        return pltpu.make_async_remote_copy(
            src_ref=full.at[core, source],
            dst_ref=full.at[core, source],
            send_sem=c_send.at[source],
            recv_sem=ag_recv.at[source * 2 + core],
            device_id=partner,
            device_id_type=MESH,
        )

    halve().start()
    halve().wait_recv()
    for p in range(4):
        both[p] = (panel[c, p].astype(jnp.float32) + half[p].astype(jnp.float32)).astype(
            jnp.bfloat16
        )
    for dz in range(3):
        scatter(dz, zl).start()
    total = both[zl].astype(jnp.float32)
    for dz in (2, 1, 0):
        with jax.named_scope("rs_wait"):
            scatter(dz, there(dz)).wait_recv()
        total += pieces[there(dz)].astype(jnp.float32)
    full[c, zl] = total.astype(jnp.bfloat16)
    for dz in range(3):
        share(dz, zl).start()
    copy_over(c, zl).start()

    def lend(g, way, source):
        spot = (lax.rem(source, 2), source // 2)
        return pltpu.make_async_remote_copy(
            src_ref=full.at[spot],
            dst_ref=theirs.at[g, way].at[spot],
            send_sem=p_send.at[g, way, source],
            recv_sem=p_recv.at[g, way, source],
            device_id=step(g, way),
            device_id_type=MESH,
        )

    def lend_all(source):
        for g in range(2):
            for way in range(2):
                lend(g, way, source).start()

    lend_all(here)
    for dz, core in ((3, 1), (2, 0), (2, 1), (1, 0), (0, 0), (1, 1), (0, 1)):
        source = there(dz)
        with jax.named_scope("ag_wait"):
            if core:
                copy_over(1 - c, source).wait_recv()
                lend_all(source * 2 + 1 - c)
            else:
                share(dz, source).wait_recv()
                copy_over(c, source).start()
                lend_all(source * 2 + c)

    def turned(n, source):
        for h in range(2):
            whole = jnp.concatenate(
                [source[h, p].astype(jnp.float32) for p in range(4)]
                + [jnp.zeros((384 - 4 * PIECE, H), jnp.float32)],
                axis=0,
            )
            seed_t[n, h] = whole.T.astype(jnp.bfloat16)

    turned(0, full)

    def c_of(n, h, series):
        cross = jnp.dot(seed_t[n, h][:, :TP], series, preferred_element_type=jnp.float32)
        return clipped(cross)

    def z_of(n, h, series):
        return fisher(c_of(n, h, series))

    slots = [(g, w) for g in range(2) for w in range(2)]

    def direct(g, j, h):
        return pltpu.make_async_remote_copy(
            src_ref=cq.at[g * 4 + j, h],
            dst_ref=gotd.at[g * 4 + j, h],
            send_sem=d_send.at[g * 4 + j, h],
            recv_sem=d_recv.at[g * 4 + j, h],
            device_id=step(g, 1 - j % 2),
            device_id_type=MESH,
        )

    for g in range(2):
        for h in range(2):
            for j in range(LENT, 4):
                series = normed[target(g, j, 3 - 2 * (j % 2))]
                cq[g * 4 + j, h] = code(c_of(0, h, series))
        for h in range(2):
            for j in range(LENT, 4):
                direct(g, j, h).start()

    with jax.named_scope("own"):

        @pl.loop(0, 2)
        def _(jj):
            for g, w in slots:
                j = 2 * jj + w
                for h in range(2):
                    zf[g * 4 + j, h] = z_of(0, h, normed[target(g, j, 1 + 2 * w)])

    def borrow(g):
        for way in range(2):
            with jax.named_scope("lendwait"):
                for source in range(8):
                    lend(g, way, source).wait_recv()
            turned(1 + 2 * g + way, theirs.at[g, way])

    def summed(g, j, h):
        return pltpu.make_async_remote_copy(
            src_ref=m3.at[g * 4 + j, h],
            dst_ref=got.at[g * 4 + j, h],
            send_sem=a_send.at[g * 4 + j, h],
            recv_sem=a_recv.at[g * 4 + j, h],
            device_id=step(g, j % 2),
            device_id_type=MESH,
        )

    def came(g, j, kind):
        return leaf(g * 4 + j, kind, 0, step(g, 0))

    def far(g, h):
        if h == 0:
            for j in range(4):
                came(g, j, 0).wait_recv()
        for j in range(4):
            i, w = g * 4 + j, j % 2
            m3[i, h] = encode(zf[i, h] + z_of(1 + 2 * g + w, h, tiles[i, 0]), 2)
        for j in range(4):
            summed(g, j, h).start()

    def near(g, h):
        for j in range(4):
            if h == 0 and j < LENT:
                came(g, j, 1).wait_recv()
            if j >= LENT:
                direct(g, j, h).wait_recv()
        for j in range(4):
            i, w = g * 4 + j, j % 2
            if j < LENT:
                term = z_of(2 + 2 * g - w, h, tiles[i, 1])
            else:
                term = fisher(plain(gotd[i, h]))
            s1[i, h] = z_of(0, h, normed[target(g, j, 0)]) + term

    rows = (slice(0, Q), slice(Q, H))

    def message2(g, h, way, kind):
        return pltpu.make_async_remote_copy(
            src_ref=s1m.at[g, h, way] if kind == 2 else s1q.at[g, h, way, kind],
            dst_ref=relay2.at[g, h, way] if kind == 0 else got2.at[g, h, way, kind - 1],
            send_sem=b_send.at[g, h, way, kind],
            recv_sem=b_recv.at[g, h, way, kind],
            device_id=step(1 - g, way),
            device_id_type=MESH,
        )

    def add_in(g, h, j):
        with jax.named_scope("m3wait"):
            summed(g, j, h).wait_recv()
        s1[g * 4 + j, h] += decode(got[g * 4 + j, h], 2)

    def cross_z(h, way):
        return pltpu.make_async_remote_copy(
            src_ref=s2q.at[h, way],
            dst_ref=gotz.at[h, way],
            send_sem=z_send.at[h, way],
            recv_sem=z_recv.at[h, way],
            device_id=across,
            device_id_type=MESH,
        )

    def second(g, h):
        add_in(g, h, 0)
        for way in range(2):
            s1q[g, h, way, 0] = encode(s1[g * 4, h, rows[way]], 4)
            message2(g, h, way, 0).start()
        add_in(g, h, 1)
        s1q[g, h, 0, 1] = encode(s1[g * 4 + 1, h, rows[1]], 4)
        message2(g, h, 0, 1).start()

    def third(g, h):
        add_in(g, h, 2)
        s1q[g, h, 1, 1] = encode(s1[g * 4 + 2, h, rows[0]], 4)
        message2(g, h, 1, 1).start()
        for way in range(2):
            with jax.named_scope("relaywait"):
                message2(g, h, way, 0).wait_recv()
            s1m[g, h, way] = encode(
                s1[g * 4 + 1 + way, h, rows[way]] + decode(relay2[g, h, way], 4), 8
            )
            message2(g, h, way, 2).start()
        add_in(g, h, 3)

    def finish(g, h):
        for way in range(2):
            with jax.named_scope("finwait"):
                message2(g, h, 1 - way, 1).wait_recv()
                message2(g, h, way, 2).wait_recv()
            s2[g, h, rows[way]] = (
                s1[g * 4 + 3, h, rows[way]]
                + decode(got2[g, h, 1 - way, 0], 4)
                + decode(got2[g, h, way, 1], 8)
            )
            if g == 0:
                s2q[h, way] = encode(s2[g, h, rows[way]], 16)
                cross_z(h, way).start()

    borrow(0)
    with jax.named_scope("far0"):
        far(0, 0)
        far(0, 1)
    borrow(1)
    far(1, 0)
    with jax.named_scope("near0"):
        near(0, 0)
        near(0, 1)
    second(0, 0)
    near(1, 0)
    second(0, 1)
    third(0, 0)
    far(1, 1)
    near(1, 1)
    second(1, 0)
    third(0, 1)
    finish(0, 0)
    second(1, 1)
    finish(0, 1)
    third(1, 0)
    third(1, 1)
    for h in range(2):
        finish(1, h)
        with jax.named_scope("zwait"):
            for way in range(2):
                cross_z(h, way).wait_recv()
                s2[1, h, rows[way]] = (
                    s2[1, h, rows[way]] + decode(gotz[h, way], 16)
                ) * (1.0 / SUBJECTS)
        out[:, h * H : (h + 1) * H] = s2[1, h].T

    halve().wait_send()
    for dz in range(3):
        scatter(dz, zl).wait_send()
        share(dz, zl).wait_send()
    for source in range(4):
        copy_over(c, source).wait_send()
    for g in range(2):
        for way in range(2):
            for source in range(8):
                lend(g, way, source).wait_send()
            for h in range(2):
                for kind in range(3):
                    message2(g, h, way, kind).wait_send()
        for j in range(4):
            came(g, j, 0).wait_send()
            if j < LENT:
                came(g, j, 1).wait_send()
            for h in range(2):
                summed(g, j, h).wait_send()
                if j >= LENT:
                    direct(g, j, h).wait_send()
    for h in range(2):
        for way in range(2):
            cross_z(h, way).wait_send()


def body(bold_series, seed_index):
    bf16, f32, i16 = jnp.bfloat16, jnp.float32, jnp.int16
    dma = pltpu.SemaphoreType.DMA
    return pl.pallas_call(
        kernel,
        out_shape=jax.ShapeDtypeStruct((TILE, K), f32),
        in_specs=[
            pl.BlockSpec(memory_space=pltpu.HBM),
            pl.BlockSpec(memory_space=pltpu.HBM),
        ],
        out_specs=pl.BlockSpec(memory_space=pltpu.VMEM),
        scratch_shapes=[
            pltpu.VMEM((1, K), jnp.int32),
            pltpu.VMEM((4, 2, T, W), f32),
            pltpu.VMEM((V // TILE, TP, TILE), bf16),
            pltpu.VMEM((4 * PIECE, K), f32),
            pltpu.VMEM((2, 4, PIECE, H), bf16),
            pltpu.VMEM((4, PIECE, H), bf16),
            pltpu.VMEM((4, PIECE, H), bf16),
            pltpu.VMEM((4, PIECE, H), bf16),
            pltpu.VMEM((2, 4, PIECE, H), bf16),
            pltpu.VMEM((2, 2, 2, 4, PIECE, H), bf16),
            pltpu.VMEM((5, 2, H, 384), bf16),
            pltpu.VMEM((8, 2, TP, TILE), bf16),
            pltpu.VMEM((8, 2, H, TILE), f32),
            pltpu.VMEM((8, 2, H, TILE), i16),
            pltpu.VMEM((8, 2, H, TILE), i16),
            pltpu.VMEM((8, 2, H, TILE), i16),
            pltpu.VMEM((8, 2, H, TILE), i16),
            pltpu.VMEM((8, 2, H, TILE), f32),
            pltpu.VMEM((2, 2, 2, 2, Q, TILE), i16),
            pltpu.VMEM((2, 2, 2, Q, TILE), i16),
            pltpu.VMEM((2, 2, 2, Q, TILE), i16),
            pltpu.VMEM((2, 2, 2, 2, Q, TILE), i16),
            pltpu.VMEM((2, 2, H, TILE), f32),
            pltpu.VMEM((2, 2, Q, TILE), i16),
            pltpu.VMEM((2, 2, Q, TILE), i16),
            dma,
            dma((4, 2)),
            dma, dma,
            dma((3,)), dma((4,)), dma((3,)), dma((8,)), dma((4,)),
            dma((2, 2, 8)), dma((2, 2, 8)), dma((8, 2)), dma((8, 2)),
            dma((8, 2)), dma((8, 2)), dma((8, 2)), dma((8, 2)),
            dma((2, 2, 2, 3)), dma((2, 2, 2, 3)),
            dma((2, 2)), dma((2, 2)),
        ],
        compiler_params=pltpu.CompilerParams(
            collective_id=0, has_side_effects=True, vmem_limit_bytes=50 * 2**20
        ),
        name="group_z",
    )(bold_series.reshape(T, 1, V), pltpu.with_memory_space_constraint(seed_index.reshape(1, K), pltpu.HBM))


def solution(mesh):
    split = Mesh(mesh.devices.reshape(4, 2, 4, 4, 2), AXES)
    return jax.shard_map(
        body,
        mesh=split,
        in_specs=(P(SUBJ, None, VOX), P()),
        out_specs=P(VOX + SUBJ, None),
        check_vma=False,
    )
```

```python
import functools

import jax
import jax.numpy as jnp
from jax import lax
from jax.experimental import pallas as pl
from jax.experimental.pallas import tpu as pltpu
from jax.sharding import Mesh
from jax.sharding import PartitionSpec as P

AXES = ("x", "zh", "y", "zl", "c")
SUBJ = ("x", "zh", "y")
VOX = ("zl", "c")

CLIP = 0.99
EPS = 1e-05
LIMIT = 2.6466525

T = 300
TP = 304
PIECE = 80
V = 8192
K = 256
LENT = 3
TILE = 256
W = 1024
B = 512
H = K // 2
Q = K // 4
SUBJECTS = 32

MESH = pl.DeviceIdType.MESH


def step_of(terms):
    return 32700.0 / (terms * LIMIT) ** 0.5


def encode(z, terms):
    root = z * lax.rsqrt(jnp.maximum(jnp.abs(z), 1e-30))
    return jnp.round(root * step_of(terms)).astype(jnp.int32).astype(jnp.int16)


def code(c):
    return jnp.round(c * (32700.0 / CLIP)).astype(jnp.int32).astype(jnp.int16)


def plain(q):
    return q.astype(jnp.int32).astype(jnp.float32) * (CLIP / 32700.0)


def decode(q, terms):
    r = q.astype(jnp.int32).astype(jnp.float32)
    return r * jnp.abs(r) * (1.0 / step_of(terms) ** 2)


def clipped(cross):
    return jnp.clip(cross * (1.0 / T), -CLIP, CLIP)


def fisher(c):
    return 0.5 * (jnp.log(1.0 + c) - jnp.log(1.0 - c))


def kernel(
    bold, seeds, out,
    chosen_seeds, raw, normed, acc, panel, half, both, pieces, full, theirs, seed_t, tiles,
    zf, m3, got, cq, gotd, s1, s1q, s1m, relay2, got2, s2, s2q, gotz,
    seed_sem, load_sem, h_send, h_recv, rs_send, rs_recv, ag_send, ag_recv, c_send, p_send, p_recv, t_send, t_recv,
    a_send, a_recv, d_send, d_recv, b_send, b_recv, z_send, z_recv,
):
    x, zh, y, zl, c = (lax.axis_index(a) for a in AXES)
    side, place = zl // 2, lax.rem(zl, 2)

    def there(dz):
        return (3 - 3 * side, 2 - side, side * 2 + 1 - place, zl)[dz]

    def step(g, way):
        return ({"x": lax.rem(x + 1 + 2 * way, 4)}, {"y": lax.rem(y + 1 + 2 * way, 4)})[g]

    across = {"zh": 1 - zh}

    barrier = pltpu.get_barrier_semaphore()
    everyone = [{"zl": there(dz)} for dz in range(3)] + [{"c": 1 - c}]
    everyone += [step(g, way) for g in range(2) for way in range(2)] + [across]
    for other in everyone:
        pl.semaphore_signal(barrier, inc=1, device_id=other, device_id_type=MESH)

    def turn(j):
        if isinstance(j, int):
            return (2, 1, 3, 0)[j]
        return lax.rem(2 - j + 3 * (j // 2) + 2 * (j // 3), 4)

    def plane(g):
        return lax.rem(zh + 1 + g, 2)

    def target(g, j, off):
        if g == 0:
            xt, yt = lax.rem(x + off, 4), lax.rem(y + turn(j), 4)
        else:
            xt, yt = lax.rem(x + turn(j), 4), lax.rem(y + off, 4)
        return (xt * 2 + plane(g)) * 4 + yt

    def line(p, g):
        return lax.rem(x + turn(p), 4) * 2 + plane(g)

    def load(p, g, j):
        first = pl.multiple_of(line(p, g) * W + j * B, B)
        return pltpu.make_async_copy(
            bold.at[:, 0, pl.ds(first, B)],
            raw.at[p, g, :, pl.ds(j * B, B)],
            load_sem.at[p, g, j],
        )

    seed_copy = pltpu.make_async_copy(seeds, chosen_seeds, seed_sem)
    seed_copy.start()

    @pl.loop(0, 4)
    def _(p):
        for g in range(2):
            for j in range(W // B):
                load(p, g, j).start()

    acc[...] = jnp.zeros_like(acc)

    def normalize(p, g):
        for j in range(W // B):
            if (p, g) == (0, 0):
                load(p, g, j).wait()
            series = raw[p, g, :, j * B : (j + 1) * B]
            center = series - jnp.sum(series, axis=0, keepdims=True) * (1.0 / T)
            spread = jnp.sum(center * center, axis=0, keepdims=True) * (1.0 / T)
            result = (center * lax.rsqrt(spread + EPS)).astype(jnp.bfloat16)
            for k in range(B // TILE):
                s = line(p, g) * 4 + j * (B // TILE) + k
                normed[s, T - T % 16 :] = jnp.zeros((TP - T + T % 16, TILE), jnp.bfloat16)
                normed[s, :T] = result[:, k * TILE : (k + 1) * TILE]

    def pick(p, g):
        ids = lax.broadcasted_iota(jnp.int32, (W, K), 0)
        wanted = chosen_seeds[...] - (zl * 2 + c) * V - line(p, g) * W
        chosen = jnp.where(ids == wanted, 1.0, 0.0).astype(jnp.bfloat16)
        total = acc[:TP]
        for k in range(W // TILE):
            total += jnp.dot(
                normed[line(p, g) * 4 + k],
                chosen[k * TILE : (k + 1) * TILE],
                preferred_element_type=jnp.float32,
            )
        acc[:TP] = total

    def leaf(i, kind, s, to):
        return pltpu.make_async_remote_copy(
            src_ref=normed.at[s],
            dst_ref=tiles.at[i, kind],
            send_sem=t_send.at[i, kind],
            recv_sem=t_recv.at[i, kind],
            device_id=to,
            device_id_type=MESH,
        )

    seed_copy.wait()

    def give(p, g):
        if g == 1:
            leaf(4 + p, 0, target(1, p, 2), step(1, p % 2)).start()
            if p < LENT:
                leaf(4 + p, 1, target(1, p, 3 - 2 * (p % 2)), step(1, 1 - p % 2)).start()
        elif p == 0:
            for j in range(4):
                leaf(j, 0, target(0, j, 2), step(0, j % 2)).start()
        elif p < 3:
            for j in range(2 - p, LENT, 2):
                leaf(j, 1, target(0, j, 2 * p - 1), step(0, p - 1)).start()

    order = [(p, g) for p in range(4) for g in range(2)]
    for n, (p, g) in enumerate(order):
        if n:
            for j in range(W // B):
                load(p, g, j).wait()
        if n:
            pick(*order[n - 1])
        normalize(p, g)
        if n == 0:
            with jax.named_scope("barrier"):
                pl.semaphore_wait(barrier, len(everyone))
        give(p, g)
    pick(*order[-1])

    for h in range(2):
        for p in range(4):
            panel[h, p] = acc[p * PIECE : (p + 1) * PIECE, h * H : (h + 1) * H].astype(
                jnp.bfloat16
            )

    here = zl * 2 + c

    partner = {"c": 1 - c}

    def halve():
        return pltpu.make_async_remote_copy(
            src_ref=panel.at[1 - c],
            dst_ref=half,
            send_sem=h_send,
            recv_sem=h_recv,
            device_id=partner,
            device_id_type=MESH,
        )

    def scatter(dz, source):
        return pltpu.make_async_remote_copy(
            src_ref=both.at[there(dz)],
            dst_ref=pieces.at[source],
            send_sem=rs_send.at[dz],
            recv_sem=rs_recv.at[source],
            device_id={"zl": there(dz)},
            device_id_type=MESH,
        )

    def share(dz, source):
        return pltpu.make_async_remote_copy(
            src_ref=full.at[c, zl],
            dst_ref=full.at[c, source],
            send_sem=ag_send.at[dz],
            recv_sem=ag_recv.at[source * 2 + c],
            device_id={"zl": there(dz)},
            device_id_type=MESH,
        )

    def copy_over(core, source):
        return pltpu.make_async_remote_copy(
            src_ref=full.at[core, source],
            dst_ref=full.at[core, source],
            send_sem=c_send.at[source],
            recv_sem=ag_recv.at[source * 2 + core],
            device_id=partner,
            device_id_type=MESH,
        )

    halve().start()
    halve().wait_recv()
    for p in range(4):
        both[p] = (panel[c, p].astype(jnp.float32) + half[p].astype(jnp.float32)).astype(
            jnp.bfloat16
        )
    for dz in range(3):
        scatter(dz, zl).start()
    total = both[zl].astype(jnp.float32)
    for dz in (2, 1, 0):
        with jax.named_scope("rs_wait"):
            scatter(dz, there(dz)).wait_recv()
        total += pieces[there(dz)].astype(jnp.float32)
    full[c, zl] = total.astype(jnp.bfloat16)
    for dz in range(3):
        share(dz, zl).start()
    copy_over(c, zl).start()

    def lend(g, way, source):
        spot = (lax.rem(source, 2), source // 2)
        return pltpu.make_async_remote_copy(
            src_ref=full.at[spot],
            dst_ref=theirs.at[g, way].at[spot],
            send_sem=p_send.at[g, way, source],
            recv_sem=p_recv.at[g, way, source],
            device_id=step(g, way),
            device_id_type=MESH,
        )

    def lend_all(source):
        for g in range(2):
            for way in range(2):
                lend(g, way, source).start()

    lend_all(here)
    for dz, core in ((3, 1), (2, 0), (2, 1), (1, 0), (0, 0), (1, 1), (0, 1)):
        source = there(dz)
        with jax.named_scope("ag_wait"):
            if core:
                copy_over(1 - c, source).wait_recv()
                lend_all(source * 2 + 1 - c)
            else:
                share(dz, source).wait_recv()
                copy_over(c, source).start()
                lend_all(source * 2 + c)

    def turned(n, source):
        for h in range(2):
            whole = jnp.concatenate(
                [source[h, p].astype(jnp.float32) for p in range(4)]
                + [jnp.zeros((384 - 4 * PIECE, H), jnp.float32)],
                axis=0,
            )
            seed_t[n, h] = whole.T.astype(jnp.bfloat16)

    turned(0, full)

    def c_of(n, h, series):
        cross = jnp.dot(seed_t[n, h][:, :TP], series, preferred_element_type=jnp.float32)
        return clipped(cross)

    def z_of(n, h, series):
        return fisher(c_of(n, h, series))

    slots = [(g, w) for g in range(2) for w in range(2)]

    def direct(g, j, h):
        return pltpu.make_async_remote_copy(
            src_ref=cq.at[g * 4 + j, h],
            dst_ref=gotd.at[g * 4 + j, h],
            send_sem=d_send.at[g * 4 + j, h],
            recv_sem=d_recv.at[g * 4 + j, h],
            device_id=step(g, 1 - j % 2),
            device_id_type=MESH,
        )

    for g in range(2):
        for h in range(2):
            for j in range(LENT, 4):
                series = normed[target(g, j, 3 - 2 * (j % 2))]
                cq[g * 4 + j, h] = code(c_of(0, h, series))
        for h in range(2):
            for j in range(LENT, 4):
                direct(g, j, h).start()

    with jax.named_scope("own"):

        @pl.loop(0, 2)
        def _(jj):
            for g, w in slots:
                j = 2 * jj + w
                for h in range(2):
                    zf[g * 4 + j, h] = z_of(0, h, normed[target(g, j, 1 + 2 * w)])

    def borrow(g):
        for way in range(2):
            with jax.named_scope("lendwait"):
                for source in range(8):
                    lend(g, way, source).wait_recv()
            turned(1 + 2 * g + way, theirs.at[g, way])

    def summed(g, j, h):
        return pltpu.make_async_remote_copy(
            src_ref=m3.at[g * 4 + j, h],
            dst_ref=got.at[g * 4 + j, h],
            send_sem=a_send.at[g * 4 + j, h],
            recv_sem=a_recv.at[g * 4 + j, h],
            device_id=step(g, j % 2),
            device_id_type=MESH,
        )

    def came(g, j, kind):
        return leaf(g * 4 + j, kind, 0, step(g, 0))

    def far(g, h):
        if h == 0:
            for j in range(4):
                came(g, j, 0).wait_recv()
        for j in range(4):
            i, w = g * 4 + j, j % 2
            m3[i, h] = encode(zf[i, h] + z_of(1 + 2 * g + w, h, tiles[i, 0]), 2)
        for j in range(4):
            summed(g, j, h).start()

    def near(g, h):
        for j in range(4):
            if h == 0 and j < LENT:
                came(g, j, 1).wait_recv()
            if j >= LENT:
                direct(g, j, h).wait_recv()
        for j in range(4):
            i, w = g * 4 + j, j % 2
            if j < LENT:
                term = z_of(2 + 2 * g - w, h, tiles[i, 1])
            else:
                term = fisher(plain(gotd[i, h]))
            s1[i, h] = z_of(0, h, normed[target(g, j, 0)]) + term

    rows = (slice(0, Q), slice(Q, H))

    def message2(g, h, way, kind):
        return pltpu.make_async_remote_copy(
            src_ref=s1m.at[g, h, way] if kind == 2 else s1q.at[g, h, way, kind],
            dst_ref=relay2.at[g, h, way] if kind == 0 else got2.at[g, h, way, kind - 1],
            send_sem=b_send.at[g, h, way, kind],
            recv_sem=b_recv.at[g, h, way, kind],
            device_id=step(1 - g, way),
            device_id_type=MESH,
        )

    def add_in(g, h, j):
        with jax.named_scope("m3wait"):
            summed(g, j, h).wait_recv()
        s1[g * 4 + j, h] += decode(got[g * 4 + j, h], 2)

    def cross_z(h, way):
        return pltpu.make_async_remote_copy(
            src_ref=s2q.at[h, way],
            dst_ref=gotz.at[h, way],
            send_sem=z_send.at[h, way],
            recv_sem=z_recv.at[h, way],
            device_id=across,
            device_id_type=MESH,
        )

    def second(g, h):
        add_in(g, h, 0)
        for way in range(2):
            s1q[g, h, way, 0] = encode(s1[g * 4, h, rows[way]], 4)
            message2(g, h, way, 0).start()
        add_in(g, h, 1)
        s1q[g, h, 0, 1] = encode(s1[g * 4 + 1, h, rows[1]], 4)
        message2(g, h, 0, 1).start()

    def third(g, h):
        add_in(g, h, 2)
        s1q[g, h, 1, 1] = encode(s1[g * 4 + 2, h, rows[0]], 4)
        message2(g, h, 1, 1).start()
        for way in range(2):
            with jax.named_scope("relaywait"):
                message2(g, h, way, 0).wait_recv()
            s1m[g, h, way] = encode(
                s1[g * 4 + 1 + way, h, rows[way]] + decode(relay2[g, h, way], 4), 8
            )
            message2(g, h, way, 2).start()
        add_in(g, h, 3)

    def finish(g, h):
        for way in range(2):
            with jax.named_scope("finwait"):
                message2(g, h, 1 - way, 1).wait_recv()
                message2(g, h, way, 2).wait_recv()
            s2[g, h, rows[way]] = (
                s1[g * 4 + 3, h, rows[way]]
                + decode(got2[g, h, 1 - way, 0], 4)
                + decode(got2[g, h, way, 1], 8)
            )
            if g == 0:
                s2q[h, way] = encode(s2[g, h, rows[way]], 16)
                cross_z(h, way).start()

    borrow(0)
    with jax.named_scope("far0"):
        far(0, 0)
        far(0, 1)
    borrow(1)
    far(1, 0)
    with jax.named_scope("near0"):
        near(0, 0)
        near(0, 1)
    second(0, 0)
    near(1, 0)
    second(0, 1)
    third(0, 0)
    far(1, 1)
    near(1, 1)
    second(1, 0)
    third(0, 1)
    finish(0, 0)
    second(1, 1)
    finish(0, 1)
    third(1, 0)
    third(1, 1)
    for h in range(2):
        finish(1, h)
        with jax.named_scope("zwait"):
            for way in range(2):
                cross_z(h, way).wait_recv()
                s2[1, h, rows[way]] = (
                    s2[1, h, rows[way]] + decode(gotz[h, way], 16)
                ) * (1.0 / SUBJECTS)
        out[:, h * H : (h + 1) * H] = s2[1, h].T

    halve().wait_send()
    for dz in range(3):
        scatter(dz, zl).wait_send()
        share(dz, zl).wait_send()
    for source in range(4):
        copy_over(c, source).wait_send()
    for g in range(2):
        for way in range(2):
            for source in range(8):
                lend(g, way, source).wait_send()
            for h in range(2):
                for kind in range(3):
                    message2(g, h, way, kind).wait_send()
        for j in range(4):
            came(g, j, 0).wait_send()
            if j < LENT:
                came(g, j, 1).wait_send()
            for h in range(2):
                summed(g, j, h).wait_send()
                if j >= LENT:
                    direct(g, j, h).wait_send()
    for h in range(2):
        for way in range(2):
            cross_z(h, way).wait_send()


def body(bold_series, seed_index):
    bf16, f32, i16 = jnp.bfloat16, jnp.float32, jnp.int16
    dma = pltpu.SemaphoreType.DMA
    return pl.pallas_call(
        kernel,
        out_shape=jax.ShapeDtypeStruct((TILE, K), f32),
        in_specs=[
            pl.BlockSpec(memory_space=pltpu.HBM),
            pl.BlockSpec(memory_space=pltpu.HBM),
        ],
        out_specs=pl.BlockSpec(memory_space=pltpu.VMEM),
        scratch_shapes=[
            pltpu.VMEM((1, K), jnp.int32),
            pltpu.VMEM((4, 2, T, W), f32),
            pltpu.VMEM((V // TILE, TP, TILE), bf16),
            pltpu.VMEM((4 * PIECE, K), f32),
            pltpu.VMEM((2, 4, PIECE, H), bf16),
            pltpu.VMEM((4, PIECE, H), bf16),
            pltpu.VMEM((4, PIECE, H), bf16),
            pltpu.VMEM((4, PIECE, H), bf16),
            pltpu.VMEM((2, 4, PIECE, H), bf16),
            pltpu.VMEM((2, 2, 2, 4, PIECE, H), bf16),
            pltpu.VMEM((5, 2, H, 384), bf16),
            pltpu.VMEM((8, 2, TP, TILE), bf16),
            pltpu.VMEM((8, 2, H, TILE), f32),
            pltpu.VMEM((8, 2, H, TILE), i16),
            pltpu.VMEM((8, 2, H, TILE), i16),
            pltpu.VMEM((8, 2, H, TILE), i16),
            pltpu.VMEM((8, 2, H, TILE), i16),
            pltpu.VMEM((8, 2, H, TILE), f32),
            pltpu.VMEM((2, 2, 2, 2, Q, TILE), i16),
            pltpu.VMEM((2, 2, 2, Q, TILE), i16),
            pltpu.VMEM((2, 2, 2, Q, TILE), i16),
            pltpu.VMEM((2, 2, 2, 2, Q, TILE), i16),
            pltpu.VMEM((2, 2, H, TILE), f32),
            pltpu.VMEM((2, 2, Q, TILE), i16),
            pltpu.VMEM((2, 2, Q, TILE), i16),
            dma,
            dma((4, 2, W // B)),
            dma, dma,
            dma((3,)), dma((4,)), dma((3,)), dma((8,)), dma((4,)),
            dma((2, 2, 8)), dma((2, 2, 8)), dma((8, 2)), dma((8, 2)),
            dma((8, 2)), dma((8, 2)), dma((8, 2)), dma((8, 2)),
            dma((2, 2, 2, 3)), dma((2, 2, 2, 3)),
            dma((2, 2)), dma((2, 2)),
        ],
        compiler_params=pltpu.CompilerParams(
            collective_id=0, has_side_effects=True, vmem_limit_bytes=50 * 2**20
        ),
        name="group_z",
    )(bold_series.reshape(T, 1, V), pltpu.with_memory_space_constraint(seed_index.reshape(1, K), pltpu.HBM))


def solution(mesh):
    split = Mesh(mesh.devices.reshape(4, 2, 4, 4, 2), AXES)
    return jax.shard_map(
        body,
        mesh=split,
        in_specs=(P(SUBJ, None, VOX), P()),
        out_specs=P(VOX + SUBJ, None),
        check_vma=False,
    )
```
